32 devices in a mesh: expert: 4 (over y, core), shard: 8 (over z, x).
Axes of the slice: x: 2, y: 2, z: 4, core: 2. Of those that a mesh axis runs over, the one named last changes fastest.
Arguments:
- master_gate: float32 [128, 2048, 768], P('expert', 'shard'), may hold values from -0.125 to 0.125
- second_gate: bfloat16 [128, 2048, 768], P('expert', 'shard'), may hold values from -0.0625 to 0.0625
- master_up: float32 [128, 2048, 768], P('expert', 'shard'), may hold values from -0.125 to 0.125
- second_up: bfloat16 [128, 2048, 768], P('expert', 'shard'), may hold values from -0.0625 to 0.0625
- router_weight: float32 [2048, 128], P('shard', 'expert'), may hold values from -0.125 to 0.125
- router_gain: float32 [2048], P('shard'), may hold values from 0.25 to 1.75
Outputs:
- final_gate: bfloat16 [128, 768, 2048], P('expert', 'shard')
- final_up: bfloat16 [128, 768, 2048], P('expert', 'shard')
- serve_router: bfloat16 [2048, 128], replicated
The draws below stay inside these ranges and needn't reach their ends.
All inputs are finite; a program needn't handle non-finite values.
Results may differ from the reference program's by a relative error of at most 0.001.
Values may be sent and summed in bfloat16 or wider, within the bound.
No kernel may reach another device: no remote copies, remote signals or barrier semaphores. Data moves between devices by JAX's collectives and lax.ppermute only.
A program may use at most 192 MiB of HBM per device.

```python
import jax
import jax.numpy as jnp

EXPERTS = 128
D_MODEL = 2048
D_EXPERT = 768


def levels(rng, dims, split, low, high):
    def one(position, shards_of):
        draws = jax.random.uniform(jax.random.fold_in(jax.random.fold_in(rng, 6), position), (shards_of,), jnp.float32, low / len(split), high / len(split))
        return jnp.repeat(jnp.exp(draws), dims[position] // shards_of).reshape((-1,) + (1,) * (len(dims) - position - 1))

    gain = one(*split[0])
    for cut in split[1:]:
        gain = gain * one(*cut)
    return gain


def scatter_about(stream_key, shape, spread, most, cuts=(), held_as=jnp.bfloat16):
    array = jax.random.normal(stream_key, shape, jnp.float32) * spread
    if len(cuts) > 0:
        array = levels(stream_key, shape, cuts, -0.22, 0.18) * array
    return jnp.clip(array, min=-most, max=most).astype(held_as)


def setup_inputs(seed: int = 0) -> dict:
    arg_keys = jax.random.split(jax.random.key(seed), 7)
    master_gate = scatter_about(arg_keys[0], (EXPERTS, D_MODEL, D_EXPERT), D_MODEL ** -0.5, 0.125, ((0, 4), (1, 8)), jnp.float32)
    second_gate = scatter_about(arg_keys[1], (EXPERTS, D_MODEL, D_EXPERT), (D_MODEL * 4) ** -0.5, 0.0625, ((0, 4), (1, 8)))
    master_up = scatter_about(arg_keys[2], (EXPERTS, D_MODEL, D_EXPERT), D_MODEL ** -0.5, 0.125, ((0, 4), (1, 8)), jnp.float32)
    second_up = scatter_about(arg_keys[3], (EXPERTS, D_MODEL, D_EXPERT), (D_MODEL * 4) ** -0.5, 0.0625, ((0, 4), (1, 8)))
    router_weight = scatter_about(arg_keys[4], (D_MODEL, EXPERTS), D_MODEL ** -0.5, 0.125, ((0, 8), (1, 4)), jnp.float32)
    router_gain = jnp.clip(1.0 + 0.15 * jax.random.normal(arg_keys[5], (D_MODEL,), jnp.float32), 0.25, 1.75)
    return dict(master_gate=master_gate, second_gate=second_gate, master_up=master_up, second_up=second_up, router_weight=router_weight, router_gain=router_gain)


def reference(master_gate, second_gate, master_up, second_up, router_weight, router_gain):
    merged_gate = master_gate + second_gate.astype(jnp.float32)
    merged_up = master_up + second_up.astype(jnp.float32)
    final_gate = merged_gate.astype(jnp.bfloat16)
    final_gate = jnp.transpose(final_gate, (0, 2, 1))
    final_up = merged_up.astype(jnp.bfloat16)
    final_up = jnp.transpose(final_up, (0, 2, 1))
    serve_router = (router_weight * router_gain[:, None]).astype(jnp.bfloat16)
    return final_gate, final_up, serve_router
```

```python
import functools

import jax
import jax.numpy as jnp
from jax import lax
from jax.experimental import pallas as pl
from jax.experimental.pallas import tpu as pltpu
from jax.sharding import PartitionSpec as P


def merge_body(ways, after, me_ref, master_ref, second_ref, *refs):
    parts, whole = refs[after:-1], refs[-1]
    served = whole.shape[0] // ways
    me = me_ref[0]
    for e in range(master_ref.shape[0]):
        merged = master_ref[e] + second_ref[e].astype(jnp.float32)
        whole[...] = merged.astype(jnp.bfloat16).T
        for k in range(ways):
            start = pl.multiple_of((me ^ k) * served, served)
            parts[k][e] = whole[pl.ds(start, served), :]


def merge(ways, me, master, second, first, last, after):
    _, rows, columns = master.shape
    count = last - first
    served = columns // ways
    step = 2 if first % 2 == 0 and count % 2 == 0 else 1
    begin = first // step
    take = pl.BlockSpec((step, rows, columns), lambda i, me: (begin + i, 0, 0))
    give = pl.BlockSpec((step, served, rows), lambda i, me: (i, 0, 0))
    size = count * rows * columns
    return pl.pallas_call(
        functools.partial(merge_body, ways, len(after)),
        grid_spec=pltpu.PrefetchScalarGridSpec(
            num_scalar_prefetch=1,
            grid=(count // step,),
            in_specs=[take, take] + [pl.BlockSpec(memory_space=pl.ANY)] * len(after),
            out_specs=[give] * ways,
            scratch_shapes=[pltpu.VMEM((columns, rows), jnp.bfloat16)],
        ),
        out_shape=[jax.ShapeDtypeStruct((count, served, rows), jnp.bfloat16)] * ways,
        compiler_params=pltpu.CompilerParams(vmem_limit_bytes=60 * 2**20),
        cost_estimate=pl.CostEstimate(flops=20 * size, bytes_accessed=8 * size, transcendentals=0),
        name="merge",
    )(me, master, second, *after)


def place_body(ways, me_ref, *refs):
    parts, out_ref = refs[:ways], refs[-1]
    rows = parts[0].shape[-1]
    me = me_ref[0]
    for k in range(ways):
        start = pl.multiple_of((me ^ k) * rows, rows)
        out_ref[:, :, pl.ds(start, rows)] = parts[k][...]


def place(ways, me, parts, experts, first, out):
    count, served, rows = parts[0].shape
    step = next(s for s in (4, 2, 1) if first % s == 0 and count % s == 0)
    begin = first // step
    take = pl.BlockSpec((step, served, rows), lambda i, me: (i, 0, 0))
    give = pl.BlockSpec((step, served, ways * rows), lambda i, me: (begin + i, 0, 0))
    size = count * served * rows * ways
    held = [] if out is None else [out]
    return pl.pallas_call(
        functools.partial(place_body, ways),
        grid_spec=pltpu.PrefetchScalarGridSpec(
            num_scalar_prefetch=1,
            grid=(count // step,),
            in_specs=[take] * ways + [pl.BlockSpec(memory_space=pl.ANY)] * len(held),
            out_specs=give,
        ),
        out_shape=jax.ShapeDtypeStruct((experts, served, ways * rows), parts[0].dtype),
        input_output_aliases={ways + 1: 0} if held else {},
        compiler_params=pltpu.CompilerParams(vmem_limit_bytes=60 * 2**20),
        cost_estimate=pl.CostEstimate(flops=5 * size, bytes_accessed=4 * size, transcendentals=0),
        name="place",
    )(me, *parts, *held)


def exchange(ways, parts):
    got = [parts[0]] + [None] * (ways - 1)
    for k in reversed(range(1, ways)):
        got[k] = lax.ppermute(parts[k], "shard", [(i, i ^ k) for i in range(ways)])
    return got


def gather_router(part_router):
    row_router = lax.all_gather(part_router, "shard", axis=0, tiled=True)
    return lax.all_gather(row_router, "expert", axis=1, tiled=True)


def plain(master, second):
    merged = (master + second.astype(jnp.float32)).astype(jnp.bfloat16)
    final = lax.all_to_all(merged, "shard", split_axis=2, concat_axis=1, tiled=True)
    return jnp.transpose(final, (0, 2, 1))


def usable(ways, experts, rows, columns):
    return rows % 128 == 0 and columns % (16 * ways) == 0 and ways & (ways - 1) == 0 and experts >= 8


def shards(ways, master_gate, second_gate, master_up, second_up, router_weight, router_gain):
    experts, rows, columns = master_gate.shape
    part_router = (router_weight * router_gain[:, None]).astype(jnp.bfloat16)
    if not usable(ways, experts, rows, columns):
        return plain(master_gate, second_gate), plain(master_up, second_up), gather_router(part_router)
    return regroup(ways, master_gate, second_gate, master_up, second_up, part_router)


def regroup(ways, master_gate, second_gate, master_up, second_up, part_router):
    experts = master_gate.shape[0]
    me = lax.axis_index("shard").astype(jnp.int32)[None]
    few = experts // 8
    gate_cuts = ((0, few), (few, experts))
    up_cuts = ((0, experts - few), (experts - few, experts))
    router_parts = exchange(ways, [part_router.T[None]] * ways)
    sides = ((master_gate, second_gate, gate_cuts), (master_up, second_up, up_cuts))
    came, after, turn = [], [], 0
    for master, second, cuts in sides:
        pieces = []
        for first, last in cuts:
            parts = merge(ways, me, master, second, first, last, after)
            after = [parts[0]]
            pieces.append((first, exchange(ways, parts)))
            turn += 1
        came.append(pieces)
    finals = []
    for pieces in came:
        out = None
        for first, parts in pieces:
            out = place(ways, me, parts, experts, first, out)
        finals.append(out)
    row_router = place(ways, me, router_parts, 1, 0, None)[0]
    serve_router = lax.all_gather(row_router, "expert", axis=0, tiled=True).T
    return finals[0], finals[1], serve_router


def solution(mesh):
    in_specs = (
        P("expert", "shard", None),
        P("expert", "shard", None),
        P("expert", "shard", None),
        P("expert", "shard", None),
        P("shard", "expert"),
        P("shard"),
    )
    out_specs = (P("expert", "shard", None), P("expert", "shard", None), P())
    ways = mesh.shape["shard"]
    return jax.shard_map(
        functools.partial(shards, ways), mesh=mesh, in_specs=in_specs, out_specs=out_specs, check_vma=False
    )
```
